8 devices in a mesh: dp: 2 (over z, y), tp: 4 (over x, core).
Axes of the slice: x: 2, y: 2, z: 1, core: 2. Of those that a mesh axis runs over, the one named last changes fastest.
Arguments:
- hidden: bfloat16 [6, 1024, 8192], P('dp', 'tp'), parts along dimension 0
- attn_gain: float32 [8192], replicated
- attn_bias: float32 [8192], replicated
- mlp_gain: float32 [8192], replicated
- mlp_bias: float32 [8192], replicated
- w_qkv: bfloat16 [8192, 8, 1152], P(None, 'tp')
- w_out: bfloat16 [8192, 8192], P('tp')
- w_up: bfloat16 [8192, 32768], P(None, 'tp')
- w_down: bfloat16 [32768, 8192], P('tp')
- positions: int32 [1024], replicated
Outputs:
- output: bfloat16 [6, 1024, 8192], P('dp', 'tp'), parts along dimension 0
There are 2 independent parts. The reference program is written for one: setup_inputs(seed, part) draws one part's arguments, and reference() takes and returns one part's arrays. A program takes and returns all parts, laid end to end along the dimension named above; an argument that names none is the same for every part.
All inputs are finite; a program needn't handle non-finite values.
Results may differ from the reference program's by a relative error of at most 0.00657843.
Values are sent between devices in bfloat16 or wider.
A program may use at most 1.5 GiB of HBM per device.

```python
import jax
import jax.numpy as jnp
from jax import lax

D = 8192
HEADS = 128
KV_HEADS = 8
HEAD = 64
FF = 32768
BATCH = 3
SEQ_LEN = 1024
QUERY_BLOCK = 64
HALF_HEAD = 32

GROUP_SIZE = HEADS // KV_HEADS
QKV_COLS = (GROUP_SIZE + 2) * HEAD


def setup_inputs(seed: int = 0, part: int = 0) -> dict:
    root_key = jax.random.key(seed)
    sub_keys = jax.random.split(root_key, 10)
    part_key = jax.random.fold_in(sub_keys[0], part)
    hidden = jax.random.normal(part_key, (BATCH, SEQ_LEN, D), jnp.float32).astype(jnp.bfloat16)
    attn_gain = 1.0 + 0.4 * jax.random.normal(sub_keys[1], (D,), jnp.float32)
    attn_bias = 0.4 * jax.random.normal(sub_keys[2], (D,), jnp.float32)
    mlp_gain = 1.0 + 0.4 * jax.random.normal(sub_keys[3], (D,), jnp.float32)
    mlp_bias = 0.4 * jax.random.normal(sub_keys[4], (D,), jnp.float32)
    w_qkv = (1.2 * D ** -0.5 * jax.random.normal(sub_keys[5], (D, KV_HEADS, QKV_COLS), jnp.float32)).astype(jnp.bfloat16)
    w_out = (2.0 * (HEADS * HEAD) ** -0.5 * jax.random.normal(sub_keys[6], (HEADS * HEAD, D), jnp.float32)).astype(jnp.bfloat16)
    w_up = (D ** -0.5 * jax.random.normal(sub_keys[7], (D, FF), jnp.float32)).astype(jnp.bfloat16)
    w_down = (FF ** -0.5 * jax.random.normal(sub_keys[8], (FF, D), jnp.float32)).astype(jnp.bfloat16)
    pos_gaps = jax.random.randint(sub_keys[9], (SEQ_LEN,), 1, 4, jnp.int32)
    positions = (jnp.cumsum(pos_gaps) - pos_gaps[0]).astype(jnp.int32)
    return {'hidden': hidden, 'attn_gain': attn_gain, 'attn_bias': attn_bias, 'mlp_gain': mlp_gain, 'mlp_bias': mlp_bias, 'w_qkv': w_qkv, 'w_out': w_out, 'w_up': w_up, 'w_down': w_down, 'positions': positions}


def layer_norm(tok_rows, norm_gain, norm_bias):
    rows32 = tok_rows.astype(jnp.float32)
    row_mean = jnp.mean(rows32, axis=-1, keepdims=True)
    centered = rows32 - row_mean
    row_var = jnp.mean(centered * centered, axis=-1, keepdims=True)
    return (centered * lax.rsqrt(row_var + 1e-5) * norm_gain + norm_bias).astype(jnp.bfloat16)


def apply_rotary(head_vals, cos_tab, sin_tab):
    vals32 = head_vals.astype(jnp.float32)
    rotated = jnp.concatenate([-vals32[..., HALF_HEAD:], vals32[..., :HALF_HEAD]], axis=-1)
    return (vals32 * cos_tab + rotated * sin_tab).astype(jnp.bfloat16)


def attend_sequence(query_rot, key_rot, value_seq):
    key32 = key_rot.astype(jnp.float32)
    value32 = value_seq.astype(jnp.float32)
    key_idx = jnp.arange(SEQ_LEN)

    def one_block(block_idx):
        row_start = block_idx * QUERY_BLOCK
        query_blk = lax.dynamic_slice_in_dim(query_rot, row_start, QUERY_BLOCK, axis=0).astype(jnp.float32)
        scores = jnp.einsum('qkgh,skh->kgqs', query_blk, key32) * HEAD ** -0.5
        query_idx = row_start + jnp.arange(QUERY_BLOCK)
        allowed = key_idx[None, :] <= query_idx[:, None]
        scores = jnp.where(allowed, scores, -1e30)
        exp_scores = jnp.exp(scores - jnp.max(scores, axis=-1, keepdims=True))
        attn_probs = (exp_scores / jnp.sum(exp_scores, axis=-1, keepdims=True)).astype(jnp.bfloat16)
        context = jnp.einsum('kgqs,skh->qkgh', attn_probs.astype(jnp.float32), value32)
        return context.astype(jnp.bfloat16)

    ctx_blocks = lax.map(one_block, jnp.arange(SEQ_LEN // QUERY_BLOCK))
    return ctx_blocks.reshape(SEQ_LEN, HEADS * HEAD)


def reference(hidden, attn_gain, attn_bias, mlp_gain, mlp_bias, w_qkv, w_out, w_up, w_down, positions):
    inv_freq = 10000.0 ** (-2.0 * jnp.arange(HALF_HEAD, dtype=jnp.float32) / HEAD)
    angles = positions.astype(jnp.float32)[:, None] * inv_freq[None, :]
    angles = jnp.concatenate([angles, angles], axis=-1)
    cos_tab = jnp.cos(angles)
    sin_tab = jnp.sin(angles)
    w_qkv_flat = w_qkv.reshape(D, KV_HEADS * QKV_COLS)

    def one_sequence(seq_rows):
        normed_attn = layer_norm(seq_rows, attn_gain, attn_bias)
        normed_mlp = layer_norm(seq_rows, mlp_gain, mlp_bias)
        qkv_rows = jnp.dot(normed_attn, w_qkv_flat, preferred_element_type=jnp.float32).astype(jnp.bfloat16)
        qkv_rows = qkv_rows.reshape(SEQ_LEN, KV_HEADS, GROUP_SIZE + 2, HEAD)
        query_rot = apply_rotary(qkv_rows[:, :, :GROUP_SIZE, :], cos_tab[:, None, None, :], sin_tab[:, None, None, :])
        key_rot = apply_rotary(qkv_rows[:, :, GROUP_SIZE, :], cos_tab[:, None, :], sin_tab[:, None, :])
        value_seq = qkv_rows[:, :, GROUP_SIZE + 1, :]
        context = attend_sequence(query_rot, key_rot, value_seq)
        attn_part = jnp.dot(context, w_out, preferred_element_type=jnp.float32)
        up_pre = jnp.dot(normed_mlp, w_up, preferred_element_type=jnp.float32)
        up_act = jax.nn.gelu(up_pre, approximate=False).astype(jnp.bfloat16)
        mlp_part = jnp.dot(up_act, w_down, preferred_element_type=jnp.float32)
        return (seq_rows.astype(jnp.float32) + attn_part + mlp_part).astype(jnp.bfloat16)

    return lax.map(one_sequence, hidden)
```

```python
import functools

import jax
import jax.numpy as jnp
from jax import lax
from jax.experimental import pallas as pl
from jax.experimental.pallas import tpu as pltpu
from jax.sharding import PartitionSpec as P


BF16 = jnp.bfloat16
F32 = jnp.float32
VMEM_LIMIT = 63 * 2 ** 20
LOG2E = 1.4426950408889634


def params(**kw):
    return pltpu.CompilerParams(vmem_limit_bytes=VMEM_LIMIT, **kw)


def norm_kernel(slab, x_ref, ag_ref, ab_ref, mg_ref, mb_ref, a_ref, m_ref):
    def body(i, carry):
        rows = pl.ds(pl.multiple_of(i * slab, slab), slab)
        x = x_ref[rows, :].astype(F32)
        width = x.shape[-1]
        mean = jnp.sum(x, axis=-1, keepdims=True) * (1.0 / width)
        cen = x - mean
        var = jnp.sum(cen * cen, axis=-1, keepdims=True) * (1.0 / width)
        hat = cen * lax.rsqrt(var + 1e-5)
        a_ref[rows, :] = (hat * ag_ref[...] + ab_ref[...]).astype(BF16)
        m_ref[rows, :] = (hat * mg_ref[...] + mb_ref[...]).astype(BF16)
        return carry

    lax.fori_loop(0, x_ref.shape[0] // slab, body, 0)


def both_norms(x, ag, ab, mg, mb):
    rows, width = x.shape
    blk = 64
    vec = pl.BlockSpec((1, width), lambda i: (0, 0))
    row = pl.BlockSpec((blk, width), lambda i: (i, 0))
    return pl.pallas_call(
        functools.partial(norm_kernel, 16),
        grid=(rows // blk,),
        out_shape=(jax.ShapeDtypeStruct(x.shape, BF16),) * 2,
        in_specs=[row, vec, vec, vec, vec],
        out_specs=(row, row),
        compiler_params=params(),
        cost_estimate=pl.CostEstimate(flops=2 * 10 ** 10, bytes_accessed=6 * x.size, transcendentals=0),
        name="norms",
    )(x, ag, ab, mg, mb)


def up_kernel(sub, x_ref, w_ref, o_ref):
    def body(i, carry):
        rows = pl.ds(pl.multiple_of(i * sub, sub), sub)
        pre = jnp.dot(x_ref[rows, :], w_ref[...], preferred_element_type=F32)
        o_ref[rows, :] = (0.5 * pre * (1.0 + lax.erf(pre * (2.0 ** -0.5)))).astype(BF16)
        return carry

    lax.fori_loop(0, x_ref.shape[0] // sub, body, 0)


def up_gelu(x, w):
    rows, depth = x.shape
    cols = w.shape[1]
    bn = 512
    return pl.pallas_call(
        functools.partial(up_kernel, 384),
        grid=(cols // bn,),
        out_shape=jax.ShapeDtypeStruct((rows, cols), BF16),
        in_specs=[
            pl.BlockSpec((rows, depth), lambda j: (0, 0), pipeline_mode=pl.Buffered(1)),
            pl.BlockSpec((depth, bn), lambda j: (0, j)),
        ],
        out_specs=pl.BlockSpec((rows, bn), lambda j: (0, j)),
        compiler_params=params(),
        cost_estimate=pl.CostEstimate(flops=2 * rows * depth * cols, bytes_accessed=2 * (x.size + w.size + rows * cols), transcendentals=rows * cols),
        name="up_gelu",
    )(x, w)


def rotate(vals, cos, sin, low):
    turned = jnp.where(low, pltpu.roll(vals, 96, 1), pltpu.roll(vals, 32, 1))
    return vals * cos + turned * sin


def attn_kernel(blk, scale, tp_ref, r0, r1, r2, r3, cq_ref, sq_ref, ck_ref, sk_ref, o_ref, q_ref, kt_ref, v_ref):
    t = pl.program_id(2)
    slots = (r0, r1, r2, r3)
    pairs = o_ref.shape[-1] // 128
    lane = lax.broadcasted_iota(jnp.int32, (blk, 128), 1)
    low = lax.rem(lane, 64) < 32
    first = lane < 64

    @pl.when(t == 0)
    def _():
        for k, ref in enumerate(slots):
            at = pl.multiple_of((tp_ref[0] ^ k) * blk, blk)
            rows = pl.ds(at, blk)
            kv = rotate(ref[0, 0, :, pairs * 128:].astype(F32), ck_ref[rows, :], sk_ref[rows, :], low)
            kv = kv.astype(BF16).astype(F32)
            swapped = pltpu.roll(kv, 64, 1)
            kt_ref[0, :, rows] = jnp.transpose(jnp.where(first, kv, 0.0)).astype(BF16)
            kt_ref[1, :, rows] = jnp.transpose(jnp.where(first, 0.0, swapped)).astype(BF16)
            v_ref[0, rows, :] = jnp.where(first, swapped, 0.0).astype(BF16)
            v_ref[1, rows, :] = jnp.where(first, 0.0, kv).astype(BF16)

    for k, ref in enumerate(slots):
        @pl.when((t ^ tp_ref[0]) == k)
        def _(ref=ref):
            for p in range(pairs):
                cols = slice(p * 128, (p + 1) * 128)
                q_ref[:, cols] = rotate(ref[0, 0, :, cols].astype(F32), cq_ref[...], sq_ref[...], low).astype(BF16)

    allowed = lax.broadcasted_iota(jnp.int32, (blk, blk), 1) <= lax.broadcasted_iota(jnp.int32, (blk, blk), 0)

    for tt in range(4):
        @pl.when(t == tt)
        def _(tt=tt):
            keys = (tt + 1) * blk

            def body(p, carry):
                cols = pl.ds(pl.multiple_of(p * 128, 128), 128)
                q = q_ref[:, cols]
                ctx = None
                for e in range(2):
                    s = jnp.dot(q, kt_ref[e, :, :keys], preferred_element_type=F32)
                    diag = jnp.where(allowed, s[:, keys - blk:], -1e30)
                    s = jnp.concatenate([s[:, :keys - blk], diag], axis=1) if tt else diag
                    top = jnp.max(s, axis=-1, keepdims=True)
                    ex = jnp.exp2((s - top) * (scale * LOG2E))
                    prob = (ex * (1.0 / jnp.sum(ex, axis=-1, keepdims=True))).astype(BF16)
                    part = jnp.dot(prob, v_ref[e, :keys, :], preferred_element_type=F32)
                    ctx = part if ctx is None else ctx + part
                o_ref[0, :, cols] = ctx.astype(BF16)
                return carry

            lax.fori_loop(0, pairs, body, 0)


def attention(qkv, my, positions):
    slots = len(qkv)
    batch, groups, blk, cols = qkv[0].shape
    head = 64
    qcols = cols - 2 * head
    inv_freq = 10000.0 ** (-2.0 * jnp.arange(head // 2, dtype=F32) / head)
    ang = positions.astype(F32)[:, None] * inv_freq[None, :]
    cos, sin = jnp.cos(ang), jnp.sin(ang)
    ones, zeros = jnp.ones_like(cos), jnp.zeros_like(sin)
    cq = jnp.concatenate([cos, cos, cos, cos], axis=1)
    sq = jnp.concatenate([-sin, sin, -sin, sin], axis=1)
    ck = jnp.concatenate([cos, cos, ones, ones], axis=1)
    sk = jnp.concatenate([-sin, sin, zeros, zeros], axis=1)
    tokens = slots * blk
    tab = pl.BlockSpec((blk, 128), lambda b, g, t, tp: (t, 0))
    full = pl.BlockSpec((tokens, 128), lambda b, g, t, tp: (0, 0))
    part = pl.BlockSpec((1, 1, blk, cols), lambda b, g, t, tp: (b, g, 0, 0))
    work = batch * groups * (qcols // head) * tokens * tokens // 2
    return pl.pallas_call(
        functools.partial(attn_kernel, blk, head ** -0.5),
        grid_spec=pltpu.PrefetchScalarGridSpec(
            num_scalar_prefetch=1,
            grid=(batch, groups, slots),
            in_specs=[part] * slots + [tab, tab, full, full],
            out_specs=pl.BlockSpec((1, blk, qcols), lambda b, g, t, tp: (tp[0] ^ t, b, g)),
            scratch_shapes=[pltpu.VMEM((blk, qcols), BF16), pltpu.VMEM((2, 128, tokens), BF16), pltpu.VMEM((2, tokens, 128), BF16)],
        ),
        out_shape=jax.ShapeDtypeStruct((slots, batch * blk, groups * qcols), BF16),
        compiler_params=params(),
        cost_estimate=pl.CostEstimate(flops=1000 * work, bytes_accessed=8 * qkv[0].size, transcendentals=work),
        name="attention",
    )(my, *qkv, cq, sq, ck, sk)


def down_kernel(sub, n_add, h_ref, c_ref, wd_ref, wo_ref, *refs):
    o_ref = refs[-1]

    def body(i, carry):
        rows = pl.ds(pl.multiple_of(i * sub, sub), sub)
        acc = jnp.dot(h_ref[rows, :], wd_ref[...], preferred_element_type=F32)
        acc += jnp.dot(c_ref[0, rows, :], wo_ref[...], preferred_element_type=F32)
        for add in refs[:n_add]:
            acc += add[rows, :].astype(F32)
        o_ref[rows, :] = acc.astype(BF16)
        return carry

    lax.fori_loop(0, h_ref.shape[0] // sub, body, 0)


def down(h, ctx, slot, wd, wo, half, adds=(), into=None, wide=False):
    rows, depth = h.shape
    width = wd.shape[1]
    bn = 512
    n = width // 2 // bn
    off = half * n

    def cols_spec(is_wide):
        return pl.BlockSpec((rows, bn), (lambda j: (0, j + off)) if is_wide else (lambda j: (0, j)))

    in_specs = [
        pl.BlockSpec((rows, depth), lambda j: (0, 0), pipeline_mode=pl.Buffered(1)),
        pl.BlockSpec((1, rows, ctx.shape[2]), lambda j: (slot, 0, 0), pipeline_mode=pl.Buffered(1)),
        pl.BlockSpec((depth, bn), lambda j: (0, j + off)),
        pl.BlockSpec((wo.shape[0], bn), lambda j: (0, j + off)),
    ] + [cols_spec(w) for _, w in adds]
    args = [h, ctx, wd, wo] + [a for a, _ in adds]
    alias = {}
    if into is not None:
        in_specs.append(pl.BlockSpec(memory_space=pl.ANY))
        alias = {len(args): 0}
        args.append(into)
    return pl.pallas_call(
        functools.partial(down_kernel, 384, len(adds)),
        grid=(n,),
        out_shape=jax.ShapeDtypeStruct((rows, width if wide else width // 2), BF16),
        in_specs=in_specs,
        out_specs=cols_spec(wide),
        input_output_aliases=alias,
        compiler_params=params(),
        cost_estimate=pl.CostEstimate(flops=rows * (depth + wo.shape[0]) * width, bytes_accessed=depth * width + 4 * rows * width, transcendentals=0),
        name="down",
    )(*args)


def solution(mesh):
    def local_layer(hidden, attn_gain, attn_bias, mlp_gain, mlp_bias, w_qkv, w_out, w_up, w_down, positions):
        batch, blk, width = hidden.shape
        rows = batch * blk
        x = hidden.reshape(rows, width)
        vecs = [v.reshape(1, width) for v in (attn_gain, attn_bias, mlp_gain, mlp_bias)]
        mate = functools.partial(lax.ppermute, axis_name='tp', perm=[(i, i ^ 1) for i in range(4)])
        over = functools.partial(lax.ppermute, axis_name='tp', perm=[(i, i ^ 2) for i in range(4)])

        def qkv_of(a):
            return jnp.einsum('bsd,dkc->bksc', a.reshape(batch, blk, width), w_qkv, preferred_element_type=F32).astype(BF16)

        def after(val, dep):
            return lax.optimization_barrier((val, dep))[0]

        x2 = over(x)
        a0, m0 = both_norms(x, *vecs)
        m1 = mate(m0)
        a1 = mate(a0)
        h0 = up_gelu(m0, w_up)
        q0 = qkv_of(after(a0, h0))
        h1 = up_gelu(after(m1, q0), w_up)
        q1 = qkv_of(after(a1, h1))
        a2, m2 = both_norms(after(x2, q1), *vecs)
        m3 = mate(m2)
        a3 = mate(a2)
        h2 = up_gelu(m2, w_up)
        q2 = qkv_of(after(a2, h2))
        h3 = up_gelu(after(m3, q2), w_up)
        q3 = qkv_of(after(a3, h3))

        my = lax.axis_index('tp').astype(jnp.int32).reshape(1)
        ctx = attention([q0, q1, q2, q3], my, positions)

        last, got = h3, {}
        hs = (h0, h1, h2, h3)
        out = None
        for slot in (3, 2, 1, 0):
            for s in range(2):
                adds = ()
                if slot == 2:
                    adds = ((got[3, s], False),)
                if slot == 0:
                    adds = ((got[1, s], False), (got[2, s], False), (x, True))
                last = down(after(hs[slot], last), ctx, slot, w_down, w_out, s, adds=adds, into=out, wide=slot == 0)
                if slot == 0:
                    out = last
                else:
                    got[slot, s] = (over if slot == 2 else mate)(last)
        return out.reshape(batch, blk, width)

    return jax.shard_map(local_layer, mesh=mesh, in_specs=(P('dp', 'tp', None), P(), P(), P(), P(), P(None, 'tp', None), P('tp', None), P(None, 'tp'), P('tp', None), P()), out_specs=P('dp', 'tp', None), check_vma=False)
```

```python
import functools

import jax
import jax.numpy as jnp
from jax import lax
from jax.experimental import pallas as pl
from jax.experimental.pallas import tpu as pltpu
from jax.sharding import PartitionSpec as P


BF16 = jnp.bfloat16
F32 = jnp.float32
VMEM_LIMIT = 63 * 2 ** 20
LOG2E = 1.4426950408889634


def params(**kw):
    return pltpu.CompilerParams(vmem_limit_bytes=VMEM_LIMIT, **kw)


def norm_kernel(blk, step, x_ref, ag_ref, ab_ref, mg_ref, mb_ref, a_ref, m_ref, mean_ref, rstd_ref):
    rows, width = x_ref.shape

    def stats(i, carry):
        at = pl.ds(pl.multiple_of(i * blk, blk), blk)

        def piece(k):
            return x_ref[at, pl.ds(pl.multiple_of(k * step, step), step)].astype(F32)

        zero = jnp.zeros((blk, step), F32)
        total = lax.fori_loop(0, width // step, lambda k, acc: acc + piece(k), zero, unroll=4)
        mean = jnp.sum(total, axis=-1, keepdims=True) * (1.0 / width)

        def square(k, acc):
            cen = piece(k) - mean
            return acc + cen * cen

        total = lax.fori_loop(0, width // step, square, zero, unroll=4)
        rstd = lax.rsqrt(jnp.sum(total, axis=-1, keepdims=True) * (1.0 / width) + 1e-5)
        mean_ref[at, :] = jnp.broadcast_to(mean, (blk, 128))
        rstd_ref[at, :] = jnp.broadcast_to(rstd, (blk, 128))
        return carry

    lax.fori_loop(0, rows // blk, stats, 0)

    def scale(k, carry):
        cols = pl.ds(pl.multiple_of(k * 128, 128), 128)
        hat = (x_ref[:, cols].astype(F32) - mean_ref[...]) * rstd_ref[...]
        a_ref[:, cols] = (hat * ag_ref[:, cols] + ab_ref[:, cols]).astype(BF16)
        m_ref[:, cols] = (hat * mg_ref[:, cols] + mb_ref[:, cols]).astype(BF16)
        return carry

    lax.fori_loop(0, width // 128, scale, 0, unroll=4)


def both_norms(x, ag, ab, mg, mb):
    rows, width = x.shape
    blk = 128
    vec = pl.BlockSpec((1, width), lambda i: (0, 0))
    row = pl.BlockSpec((blk, width), lambda i: (i, 0))
    return pl.pallas_call(
        functools.partial(norm_kernel, 32, 256),
        grid=(rows // blk,),
        out_shape=(jax.ShapeDtypeStruct(x.shape, BF16),) * 2,
        in_specs=[row, vec, vec, vec, vec],
        out_specs=(row, row),
        scratch_shapes=[pltpu.VMEM((blk, 128), F32)] * 2,
        compiler_params=params(),
        cost_estimate=pl.CostEstimate(flops=2 * 10 ** 10, bytes_accessed=6 * x.size, transcendentals=0),
        name="norms",
    )(x, ag, ab, mg, mb)


def stream_rows(step, sub, copies, work):
    parts, part = copies[0]

    def cut(i, n):
        return pl.ds(pl.multiple_of(i * n, n), n)

    @pl.when(step == 0)
    def _():
        for i in range(parts):
            for src, dst, sem in copies[1:]:
                pltpu.make_async_copy(src.at[pl.ds(i * part, part), :], dst.at[pl.ds(i * part, part), :], sem.at[i]).start()

        def body(i, carry):
            for src, dst, sem in copies[1:]:
                pltpu.make_async_copy(src.at[cut(i, part), :], dst.at[cut(i, part), :], sem.at[i]).wait()
            work(cut(i, part))
            return carry

        lax.fori_loop(0, parts, body, 0)

    @pl.when(step > 0)
    def _():
        def body(i, carry):
            work(cut(i, sub))
            return carry

        lax.fori_loop(0, parts * part // sub, body, 0)


def up_kernel(sub, parts, steps, x_hbm, y_hbm, w_ref, o_ref, x_ref, sem, y_sem):
    step = pl.program_id(0)
    which = step // steps
    second = pltpu.make_async_copy(y_hbm, x_ref.at[1], y_sem)

    @pl.when(step == 1)
    def _():
        second.start()

    @pl.when(step == steps)
    def _():
        second.wait()

    def work(rows):
        pre = jnp.dot(x_ref[which, rows, :], w_ref[...], preferred_element_type=F32)
        o_ref[0, rows, :] = (0.5 * pre * (1.0 + lax.erf(pre * (2.0 ** -0.5)))).astype(BF16)

    stream_rows(step, sub, [(parts, x_ref.shape[1] // parts), (x_hbm, x_ref.at[0], sem)], work)


def up_gelu(x, y, w):
    rows, depth = x.shape
    cols = w.shape[1]
    bn = 512
    n = cols // bn
    return pl.pallas_call(
        functools.partial(up_kernel, 384, 4, n),
        grid=(2 * n,),
        out_shape=jax.ShapeDtypeStruct((2, rows, cols), BF16),
        in_specs=[
            pl.BlockSpec(memory_space=pl.ANY),
            pl.BlockSpec(memory_space=pl.ANY),
            pl.BlockSpec((depth, bn), lambda j: (0, j % n)),
        ],
        out_specs=pl.BlockSpec((1, rows, bn), lambda j: (j // n, 0, j % n)),
        scratch_shapes=[pltpu.VMEM((2, rows, depth), BF16), pltpu.SemaphoreType.DMA((4,)), pltpu.SemaphoreType.DMA],
        compiler_params=params(),
        cost_estimate=pl.CostEstimate(flops=4 * rows * depth * cols, bytes_accessed=4 * (x.size + w.size + rows * cols), transcendentals=2 * rows * cols),
        name="up_gelu",
    )(x, y, w)


def rotate(vals, cos, sin, low):
    turned = jnp.where(low, pltpu.roll(vals, 96, 1), pltpu.roll(vals, 32, 1))
    return vals * cos + turned * sin


def attn_kernel(blk, scale, tp_ref, r0, r1, r2, r3, cq_ref, sq_ref, ck_ref, sk_ref, o_ref, q_ref, kt_ref, v_ref, pr_ref):
    t = pl.program_id(2)
    slots = (r0, r1, r2, r3)
    pairs = o_ref.shape[-1] // 128
    lane = lax.broadcasted_iota(jnp.int32, (blk, 128), 1)
    low = lax.rem(lane, 64) < 32
    first = lane < 64

    @pl.when(t == 0)
    def _():
        for k, ref in enumerate(slots):
            at = pl.multiple_of((tp_ref[0] ^ k) * blk, blk)
            rows = pl.ds(at, blk)
            kv = rotate(ref[0, 0, :, pairs * 128:].astype(F32), ck_ref[rows, :], sk_ref[rows, :], low)
            kv = kv.astype(BF16).astype(F32)
            swapped = pltpu.roll(kv, 64, 1)
            kt_ref[0, :, rows] = jnp.transpose(jnp.where(first, kv, 0.0)).astype(BF16)
            kt_ref[1, :, rows] = jnp.transpose(jnp.where(first, 0.0, swapped)).astype(BF16)
            v_ref[0, rows, :] = jnp.where(first, swapped, 0.0).astype(BF16)
            v_ref[1, rows, :] = jnp.where(first, 0.0, kv).astype(BF16)

    for k, ref in enumerate(slots):
        @pl.when((t ^ tp_ref[0]) == k)
        def _(ref=ref):
            for p in range(pairs):
                cols = slice(p * 128, (p + 1) * 128)
                q_ref[:, cols] = rotate(ref[0, 0, :, cols].astype(F32), cq_ref[...], sq_ref[...], low).astype(BF16)

    allowed = lax.broadcasted_iota(jnp.int32, (blk, blk), 1) <= lax.broadcasted_iota(jnp.int32, (blk, blk), 0)

    for tt in range(4):
        @pl.when(t == tt)
        def _(tt=tt):
            keys = (tt + 1) * blk

            def soft(s, e):
                diag = jnp.where(allowed, s[:, keys - blk:], -1e30)
                s = jnp.concatenate([s[:, :keys - blk], diag], axis=1) if tt else diag
                top = jnp.max(s, axis=-1, keepdims=True)
                ex = jnp.exp2((s - top) * (scale * LOG2E))
                pr_ref[:, e * keys:(e + 1) * keys] = (ex * (1.0 / jnp.sum(ex, axis=-1, keepdims=True))).astype(BF16)

            def body(p, carry):
                cols = pl.ds(pl.multiple_of(p * 128, 128), 128)
                q = q_ref[:, cols]
                for e in range(2):
                    soft(jnp.dot(q, kt_ref[e, :, :keys], preferred_element_type=F32), e)
                vv = jnp.concatenate([v_ref[0, :keys, :], v_ref[1, :keys, :]], axis=0)
                ctx = jnp.dot(pr_ref[:, :2 * keys], vv, preferred_element_type=F32)
                o_ref[0, :, cols] = ctx.astype(BF16)
                return carry

            lax.fori_loop(0, pairs, body, 0)


def attention(qkv, my, positions):
    slots = len(qkv)
    batch, groups, blk, cols = qkv[0].shape
    head = 64
    qcols = cols - 2 * head
    inv_freq = 10000.0 ** (-2.0 * jnp.arange(head // 2, dtype=F32) / head)
    ang = positions.astype(F32)[:, None] * inv_freq[None, :]
    cos, sin = jnp.cos(ang), jnp.sin(ang)
    ones, zeros = jnp.ones_like(cos), jnp.zeros_like(sin)
    cq = jnp.concatenate([cos, cos, cos, cos], axis=1)
    sq = jnp.concatenate([-sin, sin, -sin, sin], axis=1)
    ck = jnp.concatenate([cos, cos, ones, ones], axis=1)
    sk = jnp.concatenate([-sin, sin, zeros, zeros], axis=1)
    tokens = slots * blk
    tab = pl.BlockSpec((blk, 128), lambda b, g, t, tp: (t, 0))
    full = pl.BlockSpec((tokens, 128), lambda b, g, t, tp: (0, 0))
    part = pl.BlockSpec((1, 1, blk, cols), lambda b, g, t, tp: (b, g, 0, 0))
    work = batch * groups * (qcols // head) * tokens * tokens // 2
    return pl.pallas_call(
        functools.partial(attn_kernel, blk, head ** -0.5),
        grid_spec=pltpu.PrefetchScalarGridSpec(
            num_scalar_prefetch=1,
            grid=(batch, groups, slots),
            in_specs=[part] * slots + [tab, tab, full, full],
            out_specs=pl.BlockSpec((1, blk, qcols), lambda b, g, t, tp: (tp[0] ^ t, b, g)),
            scratch_shapes=[pltpu.VMEM((blk, qcols), BF16), pltpu.VMEM((2, 128, tokens), BF16), pltpu.VMEM((2, tokens, 128), BF16)] + [pltpu.VMEM((blk, 2 * tokens), BF16)],
        ),
        out_shape=jax.ShapeDtypeStruct((slots, batch * blk, groups * qcols), BF16),
        compiler_params=params(),
        cost_estimate=pl.CostEstimate(flops=1000 * work, bytes_accessed=8 * qkv[0].size, transcendentals=work),
        name="attention",
    )(my, *qkv, cq, sq, ck, sk)


def down_kernel(sub, parts, slot, which, n_add, h_hbm, c_hbm, wd_ref, wo_ref, *refs):
    o_ref, h_ref, c_ref, h_sem, c_sem = refs[-5:]

    def work(rows):
        acc = jnp.dot(h_ref[rows, :], wd_ref[...], preferred_element_type=F32)
        acc += jnp.dot(c_ref[rows, :], wo_ref[...], preferred_element_type=F32)
        for add in refs[:n_add]:
            acc += add[rows, :].astype(F32)
        o_ref[rows, :] = acc.astype(BF16)

    copies = [(parts, h_ref.shape[0] // parts), (h_hbm.at[which], h_ref, h_sem), (c_hbm.at[slot], c_ref, c_sem)]
    stream_rows(pl.program_id(0), sub, copies, work)


def down(h, which, ctx, slot, wd, wo, half, adds=(), into=None, wide=False):
    rows, depth = h.shape[1:]
    width = wd.shape[1]
    bn = 512
    n = width // 2 // bn
    off = half * n

    def cols_spec(is_wide):
        return pl.BlockSpec((rows, bn), (lambda j: (0, j + off)) if is_wide else (lambda j: (0, j)))

    in_specs = [
        pl.BlockSpec(memory_space=pl.ANY),
        pl.BlockSpec(memory_space=pl.ANY),
        pl.BlockSpec((depth, bn), lambda j: (0, j + off)),
        pl.BlockSpec((wo.shape[0], bn), lambda j: (0, j + off)),
    ] + [cols_spec(w) for _, w in adds]
    args = [h, ctx, wd, wo] + [a for a, _ in adds]
    alias = {}
    if into is not None:
        in_specs.append(pl.BlockSpec(memory_space=pl.ANY))
        alias = {len(args): 0}
        args.append(into)
    return pl.pallas_call(
        functools.partial(down_kernel, 384, 4, slot, which, len(adds)),
        grid=(n,),
        out_shape=jax.ShapeDtypeStruct((rows, width if wide else width // 2), BF16),
        in_specs=in_specs,
        out_specs=cols_spec(wide),
        scratch_shapes=[
            pltpu.VMEM((rows, depth), BF16),
            pltpu.VMEM((rows, ctx.shape[2]), BF16),
            pltpu.SemaphoreType.DMA((4,)),
            pltpu.SemaphoreType.DMA((4,)),
        ],
        input_output_aliases=alias,
        compiler_params=params(),
        cost_estimate=pl.CostEstimate(flops=rows * (depth + wo.shape[0]) * width, bytes_accessed=depth * width + 4 * rows * width, transcendentals=0),
        name="down",
    )(*args)


def solution(mesh):
    def local_layer(hidden, attn_gain, attn_bias, mlp_gain, mlp_bias, w_qkv, w_out, w_up, w_down, positions):
        batch, blk, width = hidden.shape
        rows = batch * blk
        x = hidden.reshape(rows, width)
        vecs = [v.reshape(1, width) for v in (attn_gain, attn_bias, mlp_gain, mlp_bias)]
        mate = functools.partial(lax.ppermute, axis_name='tp', perm=[(i, i ^ 1) for i in range(4)])
        over = functools.partial(lax.ppermute, axis_name='tp', perm=[(i, i ^ 2) for i in range(4)])

        def qkv_of(a):
            return jnp.einsum('bsd,dkc->bksc', a.reshape(batch, blk, width), w_qkv, preferred_element_type=F32).astype(BF16)

        def after(val, dep):
            return lax.optimization_barrier((val, dep))[0]

        x2 = over(x)
        a0, m0 = both_norms(x, *vecs)
        m1 = mate(m0)
        a1 = mate(a0)
        q0 = qkv_of(a0)
        h01 = up_gelu(m0, after(m1, q0), w_up)
        q1 = qkv_of(after(a1, h01))
        a2, m2 = both_norms(after(x2, q1), *vecs)
        m3 = mate(m2)
        a3 = mate(a2)
        q2 = qkv_of(a2)
        h23 = up_gelu(m2, after(m3, q2), w_up)
        q3 = qkv_of(after(a3, h23))

        my = lax.axis_index('tp').astype(jnp.int32).reshape(1)
        ctx = attention([q0, q1, q2, q3], my, positions)

        last, got = h23, {}
        hs = (h01, h01, h23, h23)
        out = None
        for slot in (3, 2, 1, 0):
            for s in range(2):
                adds = ()
                if slot == 2:
                    adds = ((got[3, s], False),)
                if slot == 0:
                    adds = ((got[1, s], False), (got[2, s], False), (x, True))
                last = down(after(hs[slot], last), slot % 2, ctx, slot, w_down, w_out, s, adds=adds, into=out, wide=slot == 0)
                if slot == 0:
                    out = last
                else:
                    got[slot, s] = (over if slot == 2 else mate)(last)
        return out.reshape(batch, blk, width)

    return jax.shard_map(local_layer, mesh=mesh, in_specs=(P('dp', 'tp', None), P(), P(), P(), P(), P(None, 'tp', None), P('tp', None), P(None, 'tp'), P('tp', None), P()), out_specs=P('dp', 'tp', None), check_vma=False)
```
